16 devices in a mesh: rep: 2 (over y, z), dp: 8 (over x, core).
Axes of the slice: x: 4, y: 2, z: 1, core: 2. Of those that a mesh axis runs over, the one named last changes fastest.
The devices are a block of a 4x4x8 slice.
Arguments:
- a: bfloat16 [16, 4, 4096, 512], P(('rep', 'dp')), parts along dimension 0
- g: bfloat16 [16, 4, 4096, 2048], P(('rep', 'dp')), parts along dimension 0
Outputs:
- output: bfloat16 [8, 512, 2048], P('rep'), parts along dimension 0
There are 2 independent parts. The reference program is written for one: setup_inputs(seed, part) draws one part's arguments, and reference() takes and returns one part's arrays. A program takes and returns all parts, laid end to end along the dimension named above; each array names one.
All inputs are finite; a program needn't handle non-finite values.
Results may differ from the reference program's by a relative error of at most 0.012.
Values are sent between devices in bfloat16 or wider.
A program may use at most 768 MiB of HBM per device.

```python
import jax
import jax.numpy as jnp
from jax import lax

DEVICES = 8
MATRICES = 4
TOKENS = 4096
D = 512
FF = 2048


def setup_inputs(seed: int = 0, part: int = 0) -> dict:
    ka, kg, ks = (jax.random.fold_in(k, part) for k in jax.random.split(jax.random.key(seed), 3))
    size = 2.0 ** jax.random.uniform(ks, (DEVICES, MATRICES, 1, 1), jnp.float32, -1.0, 1.0)
    a = jax.random.normal(ka, (DEVICES, MATRICES, TOKENS, D), jnp.float32)
    g = size * jax.random.normal(kg, (DEVICES, MATRICES, TOKENS, FF), jnp.float32) * (DEVICES * TOKENS) ** -0.5
    return {"a": a.astype(jnp.bfloat16), "g": g.astype(jnp.bfloat16)}


def reference(a, g):
    def take(so_far, one):
        return so_far + jnp.einsum("ntd,ntf->ndf", *one, preferred_element_type=jnp.float32), None

    return lax.scan(take, jnp.zeros((MATRICES, D, FF), jnp.float32), (a, g))[0].astype(jnp.bfloat16)
```

```python
import functools

import jax
import jax.numpy as jnp
from jax import lax
from jax.experimental import pallas as pl
from jax.experimental.pallas import tpu as pltpu
from jax.sharding import PartitionSpec as P

MESH = pl.DeviceIdType.MESH
BLOCK = 512
ACCS = 8
LAG2, LAG3, LAG4, LAG5 = 1, 2, 5, 8


def kernel(
    chips,
    a_hbm,
    g_hbm,
    out,
    abuf,
    gbuf,
    acc,
    give,
    take,
    stage,
    part,
    whole,
    a_sem,
    g_sem,
    give_sem,
    take_sem,
    stage_sem,
    part_sem,
    whole_sem,
    own_sem,
    near_sem,
    pass_sem,
    far_sem,
    last_sem,
    done_sem,
):
    matrices, rows, columns = out.shape
    blocks = columns // BLOCK
    pieces = matrices * blocks
    half = rows // 2
    chunk = half // chips
    h = chunk // 2

    me = lax.axis_index("dp")
    chip, core = me // 2, me % 2
    other = chip * 2 + 1 - core
    nxt, prv = (chip + 1) % chips, (chip + chips - 1) % chips
    opp = (chip + 2) % chips
    right, left = nxt * 2 + core, prv * 2 + core
    to = (right, left)

    def a_copy(n):
        return pltpu.make_async_copy(a_hbm.at[0, n], abuf.at[n % 2], a_sem.at[n % 2])

    def g_copy(p):
        cols = pl.ds(pl.multiple_of(p % blocks * BLOCK, BLOCK), BLOCK)
        return pltpu.make_async_copy(g_hbm.at[0, p // blocks, :, cols], gbuf.at[p % 3], g_sem.at[p % 3])

    def send(src, dst, send_sem, recv_sem, device):
        return pltpu.make_async_remote_copy(
            src_ref=src,
            dst_ref=dst,
            send_sem=send_sem,
            recv_sem=recv_sem,
            device_id={"dp": device},
            device_id_type=MESH,
        )

    def rows_of(first, size):
        return pl.ds(pl.multiple_of(first, h), size)

    def in_out(p, first, size):
        cols = pl.ds(pl.multiple_of(p % blocks * BLOCK, BLOCK), BLOCK)
        return out.at[p // blocks, pl.ds(pl.multiple_of(core * half + first, h), size), cols]

    def exchange(p):
        return send(give.at[p], take.at[p], give_sem, take_sem.at[p], other)

    def part_copy(p, way):
        src = stage.at[p, pl.ds(2 * chunk + way * h, h)]
        return send(src, part.at[p, way], stage_sem, part_sem.at[p, way], to[way])

    def whole_copy(p, way, piece_half):
        src = stage.at[p, pl.ds(way * chunk + piece_half * h, h)]
        dst = whole.at[p, way, pl.ds(piece_half * h, h)]
        return send(src, dst, stage_sem, whole_sem.at[p, way], to[way])

    def own_copy(p, way):
        where = in_out(p, chip * chunk, chunk)
        return send(where, where, own_sem, near_sem.at[p, way], to[way])

    def pass_copy(p, way):
        where = in_out(p, (prv, nxt)[way] * chunk + way * h, h)
        return send(where, where, pass_sem, far_sem.at[p, way], to[way])

    def last_copy(p):
        where = in_out(p, 0, half)
        return send(where, where, last_sem, done_sem, other)

    def wait_all(ref, sem):
        pltpu.make_async_copy(ref, ref, sem).wait()

    a_copy(0).start()
    g_copy(0).start()
    g_copy(1).start()

    barrier = pltpu.get_barrier_semaphore()
    for device in (other, right, left):
        pl.semaphore_signal(barrier, inc=1, device_id={"dp": device}, device_id_type=MESH)
    pl.semaphore_wait(barrier, 3)

    @pl.loop(0, pieces + LAG5)
    def _(s):
        @pl.when(s < pieces)
        def _():
            p, n, c = s, s // blocks, s % blocks

            @pl.when(p + 2 < pieces)
            def _():
                g_copy(p + 2).start()

            @pl.when((c == 0) & (n + 1 < matrices))
            def _():
                a_copy(n + 1).start()

            @pl.when(c == 0)
            def _():
                a_copy(n).wait()

            g_copy(p).wait()

            def product(owner):
                mine = pl.ds(pl.multiple_of(owner * half, half), half)
                return lax.dot_general(
                    abuf[n % 2, :, mine],
                    gbuf[p % 3],
                    (((0,), (0,)), ((), ())),
                    preferred_element_type=jnp.float32,
                )

            give[p] = product(1 - core).astype(give.dtype)
            exchange(p).start()
            acc[p % ACCS] = product(core)

        @pl.when((s >= LAG2) & (s < pieces + LAG2))
        def _():
            p = s - LAG2
            for way in range(2):
                part_copy(p, way).wait_recv()
                mine = acc[p % ACCS, rows_of((nxt, prv)[way] * chunk + way * h, h)]
                total = mine + part[p, way].astype(jnp.float32)
                stage[p, pl.ds(way * chunk + way * h, h)] = total.astype(stage.dtype)
                whole_copy(p, way, way).start()

        @pl.when(s < pieces)
        def _():
            p = s
            exchange(p).wait_recv()

            def total(first, size):
                where = rows_of(first, size)
                return acc[p % ACCS, where] + take[p, where].astype(jnp.float32)

            stage[p, pl.ds(2 * chunk, chunk)] = total(opp * chunk, chunk).astype(stage.dtype)
            for way in range(2):
                part_copy(p, way).start()
            for way in range(2):
                rest = (nxt, prv)[way] * chunk + (1 - way) * h
                stage[p, pl.ds(way * chunk + (1 - way) * h, h)] = total(rest, h).astype(stage.dtype)
                whole_copy(p, way, 1 - way).start()
            for way in range(2):
                first = (nxt, prv)[way] * chunk + way * h
                acc[p % ACCS, rows_of(first, h)] = total(first, h)
            acc[p % ACCS, rows_of(chip * chunk, chunk)] = total(chip * chunk, chunk)

        @pl.when((s >= LAG3) & (s < pieces + LAG3))
        def _():
            p = s - LAG3
            for way in range(2):
                wait = whole.at[p, way]
                send(wait, wait, stage_sem, whole_sem.at[p, way], to[way]).wait_recv()
            total = acc[p % ACCS, rows_of(chip * chunk, chunk)]
            total = total + whole[p, 0].astype(jnp.float32) + whole[p, 1].astype(jnp.float32)
            in_out(p, chip * chunk, chunk)[...] = total.astype(out.dtype)
            for way in range(2):
                own_copy(p, way).start()

        @pl.when((s >= LAG4) & (s < pieces + LAG4))
        def _():
            p = s - LAG4
            for way in range(2):
                own_copy(p, way).wait_recv()
                pass_copy(p, way).start()

        @pl.when(s >= LAG5)
        def _():
            p = s - LAG5
            for way in range(2):
                pass_copy(p, way).wait_recv()
            last_copy(p).start()

    wait_all(give, give_sem)
    wait_all(stage, stage_sem)
    wait_all(whole, own_sem)
    wait_all(part, pass_sem)
    wait_all(take, last_sem)
    wait_all(take, done_sem)


def solution(mesh):
    chips = mesh.shape["dp"] // 2

    def step(a, g):
        _, matrices, tokens, rows = a.shape
        columns = g.shape[-1]
        pieces = matrices * (columns // BLOCK)
        half = rows // 2
        chunk = half // chips
        vmem = lambda *shape: pltpu.VMEM(shape, jnp.bfloat16)
        dma = pltpu.SemaphoreType.DMA
        return pl.pallas_call(
            functools.partial(kernel, chips),
            out_shape=jax.ShapeDtypeStruct((matrices, rows, columns), jnp.bfloat16),
            in_specs=[pl.BlockSpec(memory_space=pl.ANY)] * 2,
            out_specs=pl.BlockSpec(memory_space=pltpu.VMEM),
            scratch_shapes=[
                vmem(2, tokens, rows),
                vmem(3, tokens, BLOCK),
                pltpu.VMEM((ACCS, half, BLOCK), jnp.float32),
                vmem(pieces, half, BLOCK),
                vmem(pieces, half, BLOCK),
                vmem(pieces, 3 * chunk, BLOCK),
                vmem(pieces, 2, chunk // 2, BLOCK),
                vmem(pieces, 2, chunk, BLOCK),
                dma((2,)),
                dma((3,)),
                dma,
                dma((pieces,)),
                dma,
                dma((pieces, 2)),
                dma((pieces, 2)),
                dma,
                dma((pieces, 2)),
                dma,
                dma((pieces, 2)),
                dma,
                dma,
            ],
            compiler_params=pltpu.CompilerParams(
                collective_id=0, has_side_effects=True, vmem_limit_bytes=63 * 2**20
            ),
            name="grad_sums",
        )(a, g)

    return jax.shard_map(
        step,
        mesh=mesh,
        in_specs=(P(("rep", "dp")), P(("rep", "dp"))),
        out_specs=P("rep"),
        check_vma=False,
    )
```

```python
import functools

import jax
import jax.numpy as jnp
from jax import lax
from jax.experimental import pallas as pl
from jax.experimental.pallas import tpu as pltpu
from jax.sharding import PartitionSpec as P

MESH = pl.DeviceIdType.MESH
BLOCK = 512
ACCS = 4
HEAD = 4
PARTS, WHOLES = 6, 12
SPARSE = 4
DENSE = 15, 3
GATHER = 17
CLOSE = 20

def kernel(
    chips,
    a_hbm,
    g_hbm,
    out,
    abuf,
    gbuf,
    acc,
    kept,
    give,
    take,
    stage,
    part,
    whole,
    head_sem,
    a_sem,
    g_sem,
    give_sem,
    take_sem,
    stage_sem,
    part_sem,
    whole_sem,
    own_sem,
    near_sem,
    pass_sem,
    far_sem,
    last_sem,
    done_sem,
):
    matrices, rows, columns = out.shape
    tokens = abuf.shape[1]
    blocks = columns // BLOCK
    pieces = matrices * blocks
    half = rows // 2
    chunk = half // chips
    h = chunk // 2

    me = lax.axis_index("dp")
    chip, core = me // 2, me % 2
    other = chip * 2 + 1 - core
    nxt, prv = (chip + 1) % chips, (chip + chips - 1) % chips
    opp = (chip + 2) % chips
    right, left = nxt * 2 + core, prv * 2 + core
    to = (right, left)
    beside = (nxt, prv)

    class Piece:
        def __init__(self, p):
            self.p = p
            self.n = p // blocks
            self.acc = p % ACCS
            self.cols = pl.ds(pl.multiple_of(p % blocks * BLOCK, BLOCK), BLOCK)

        def in_out(self, row, size):
            return out.at[self.n, pl.ds(pl.multiple_of(core * half + row, h), size), self.cols]

    def a_copy(n):
        return pltpu.make_async_copy(a_hbm.at[0, n], abuf.at[n % 2], a_sem.at[n % 2])

    def g_copy(p):
        cols = pl.ds(pl.multiple_of(p % blocks * BLOCK, BLOCK), BLOCK)
        return pltpu.make_async_copy(g_hbm.at[0, p // blocks, :, cols], gbuf.at[p % 3], g_sem.at[p % 3])

    def head_copies(k):
        size = tokens // HEAD
        some = pl.ds(k * size, size)
        return (
            pltpu.make_async_copy(a_hbm.at[0, 0, some], abuf.at[0, some], head_sem.at[k]),
            pltpu.make_async_copy(g_hbm.at[0, 0, some, pl.ds(0, BLOCK)], gbuf.at[0, some], head_sem.at[k]),
        )

    def send(src, dst, send_sem, recv_sem, device):
        return pltpu.make_async_remote_copy(
            src_ref=src,
            dst_ref=dst,
            send_sem=send_sem,
            recv_sem=recv_sem,
            device_id={"dp": device},
            device_id_type=MESH,
        )

    def rows_of(row, size):
        return pl.ds(pl.multiple_of(row, h), size)

    def exchange(x):
        return send(give.at[x.p], take.at[x.p], give_sem, take_sem.at[x.p % 3], other)

    def part_copy(x, way):
        src = stage.at[x.p, pl.ds(2 * chunk + way * h, h)]
        return send(src, part.at[x.p, way], stage_sem, part_sem.at[x.p % PARTS], to[way])

    def whole_copy(x, way, piece_half):
        src = stage.at[x.p, pl.ds(way * chunk + piece_half * h, h)]
        dst = whole.at[x.p, way, pl.ds(piece_half * h, h)]
        return send(src, dst, stage_sem, whole_sem.at[x.p % WHOLES], to[way])

    def own_copy(x, way):
        where = x.in_out(chip * chunk, chunk)
        return send(where, where, own_sem, near_sem.at[x.p // 2], to[way])

    def pass_copy(x, way):
        where = x.in_out((prv, nxt)[way] * chunk + way * h, h)
        return send(where, where, pass_sem, far_sem.at[x.p // 2], to[way])

    def last_copy(x, owner):
        where = x.in_out(owner * chunk, chunk)
        return send(where, where, last_sem, done_sem, other)

    def wait_all(ref, sem):
        pltpu.make_async_copy(ref, ref, sem).wait()

    def own_term(x, row, size):
        where = rows_of(row, size)
        return acc[x.acc, where] + take[x.p, where].astype(jnp.float32)

    def begin(x):
        exchange(x).wait_recv()
        stage[x.p, pl.ds(2 * chunk, chunk)] = own_term(x, opp * chunk, chunk).astype(stage.dtype)
        for way in range(2):
            part_copy(x, way).start()
        for way in range(2):
            rest = beside[way] * chunk + (1 - way) * h
            stage[x.p, pl.ds(way * chunk + (1 - way) * h, h)] = own_term(x, rest, h).astype(stage.dtype)
            whole_copy(x, way, 1 - way).start()
        for way in range(2):
            row = beside[way] * chunk + way * h
            acc[x.acc, rows_of(row, h)] = own_term(x, row, h)
        kept[x.p] = own_term(x, chip * chunk, chunk)

    def pass_parts(x):
        wait_all(part.at[x.p], part_sem.at[x.p % PARTS])
        for way in range(2):
            mine = acc[x.acc, rows_of(beside[way] * chunk + way * h, h)]
            total = mine + part[x.p, way].astype(jnp.float32)
            stage[x.p, pl.ds(way * chunk + way * h, h)] = total.astype(stage.dtype)
            whole_copy(x, way, way).start()

    def finish(x):
        wait_all(whole.at[x.p], whole_sem.at[x.p % WHOLES])
        total = kept[x.p]
        for way in range(2):
            total += whole[x.p, way].astype(jnp.float32)
        x.in_out(chip * chunk, chunk)[...] = total.astype(out.dtype)
        for way in range(2):
            own_copy(x, way).start()

    def gather(q):
        wait_all(whole.at[pl.ds(2 * q, 2)], near_sem.at[q])
        for x in (Piece(2 * q), Piece(2 * q + 1)):
            for way in range(2):
                pass_copy(x, way).start()
            for owner in (chip, nxt, prv):
                last_copy(x, owner).start()

    def close(q):
        wait_all(part.at[pl.ds(2 * q, 2)], far_sem.at[q])
        for x in (Piece(2 * q), Piece(2 * q + 1)):
            last_copy(x, opp).start()

    def when(live, do, p):
        pl.when(live & (p >= 0) & (p < pieces))(lambda: do(Piece(p)))

    def product(lhs, rhs):
        return lax.dot_general(lhs, rhs, (((0,), (0,)), ((), ())), preferred_element_type=jnp.float32)

    for k in range(HEAD):
        for copy in head_copies(k):
            copy.start()
    g_copy(1).start()
    barrier = pltpu.get_barrier_semaphore()
    for device in (other, right, left):
        pl.semaphore_signal(barrier, inc=1, device_id={"dp": device}, device_id_type=MESH)
    mine, theirs = rows_of(core * half, half), rows_of((1 - core) * half, half)

    for k in range(HEAD):
        wait_all(gbuf.at[pl.ds(0, 2), pl.ds(0, tokens // HEAD)], head_sem.at[k])
        some = pl.ds(k * (tokens // HEAD), tokens // HEAD)
        terms = product(abuf[0, some, theirs], gbuf[0, some])
        if k < HEAD - 1:
            acc[1] = terms + acc[1] if k else terms
        else:
            give[0] = (terms + acc[1]).astype(give.dtype)
            pl.semaphore_wait(barrier, 3)
            exchange(Piece(0)).start()
        terms = product(abuf[0, some, mine], gbuf[0, some])
        acc[0] = terms + acc[0] if k else terms
    g_copy(2).start()

    def nth(k):
        return k - (k + 1) // 3

    @pl.loop(1, CLOSE + pieces // 2)
    def _(s):
        p, n, c = s, s // blocks, s % blocks

        @pl.when(s < pieces)
        def _():
            @pl.when(p + 2 < pieces)
            def _():
                g_copy(p + 2).start()

            @pl.when((c == 1) & (n + 1 < matrices))
            def _():
                a_copy(n + 1).start()

            @pl.when(c == 0)
            def _():
                a_copy(n).wait()

            g_copy(p).wait()
            give[p] = product(abuf[n % 2, :, theirs], gbuf[p % 3]).astype(give.dtype)
            exchange(Piece(p)).start()

        when(s == 1, begin, 0)
        when(s > 2, pass_parts, s - 2)

        @pl.when(s < pieces)
        def _():
            acc[p % ACCS] = product(abuf[n % 2, :, mine], gbuf[p % 3])

        when(s > 0, begin, s)
        when(s == 2, pass_parts, 0)
        k = s - SPARSE
        when((s < DENSE[0]) & (k >= 0) & (k % 3 != 1), finish, nth(k))
        for i in range(DENSE[1]):
            when(s >= DENSE[0], finish, nth(DENSE[0] - SPARSE) + (s - DENSE[0]) * DENSE[1] + i)
        pl.when((s >= GATHER) & (s < GATHER + pieces // 2))(lambda: gather(s - GATHER))
        pl.when(s >= CLOSE)(lambda: close(s - CLOSE))

    wait_all(give, give_sem)
    wait_all(stage, stage_sem)
    wait_all(whole, own_sem)
    wait_all(part, pass_sem)
    wait_all(take, last_sem)
    wait_all(take, done_sem)


def solution(mesh):
    chips = mesh.shape["dp"] // 2

    def step(a, g):
        _, matrices, tokens, rows = a.shape
        columns = g.shape[-1]
        pieces = matrices * (columns // BLOCK)
        half = rows // 2
        chunk = half // chips
        vmem = lambda *shape: pltpu.VMEM(shape, jnp.bfloat16)
        dma = pltpu.SemaphoreType.DMA
        return pl.pallas_call(
            functools.partial(kernel, chips),
            out_shape=pltpu.VMEM((matrices, rows, columns), jnp.bfloat16),
            in_specs=[pl.BlockSpec(memory_space=pl.ANY)] * 2,
            out_specs=pl.BlockSpec(memory_space=pltpu.VMEM),
            scratch_shapes=[
                vmem(2, tokens, rows),
                vmem(3, tokens, BLOCK),
                pltpu.VMEM((ACCS, half, BLOCK), jnp.float32),
                pltpu.VMEM((pieces, chunk, BLOCK), jnp.float32),
                vmem(pieces, half, BLOCK),
                vmem(pieces, half, BLOCK),
                vmem(pieces, 3 * chunk, BLOCK),
                vmem(pieces, 2, chunk // 2, BLOCK),
                vmem(pieces, 2, chunk, BLOCK),
                dma((HEAD,)),
                dma((2,)),
                dma((3,)),
                dma,
                dma((3,)),
                dma,
                dma((PARTS,)),
                dma((WHOLES,)),
                dma,
                dma((pieces // 2,)),
                dma,
                dma((pieces // 2,)),
                dma,
                dma,
            ],
            compiler_params=pltpu.CompilerParams(
                collective_id=0, has_side_effects=True, vmem_limit_bytes=50 * 2**20
            ),
            name="grad_sums",
        )(a, g)

    return jax.shard_map(
        step,
        mesh=mesh,
        in_specs=(P(("rep", "dp")), P(("rep", "dp"))),
        out_specs=P("rep"),
        check_vma=False,
    )
```

```python
import functools

import jax
import jax.numpy as jnp
from jax import lax
from jax.experimental import pallas as pl
from jax.experimental.pallas import tpu as pltpu
from jax.sharding import PartitionSpec as P

MESH = pl.DeviceIdType.MESH
BLOCK = 512
ACCS = 4
HEAD = 2, 2, 2, 2
PARTS, WHOLES = 6, 9
SPARSE = 3
DENSE = 15, 2
GATHER = 18
CLOSE = 21

def kernel(
    chips,
    a_hbm,
    g_hbm,
    out,
    abuf,
    gbuf,
    acc,
    kept,
    give,
    take,
    stage,
    part,
    whole,
    head_sem,
    a_sem,
    g_sem,
    give_sem,
    take_sem,
    stage_sem,
    part_sem,
    whole_sem,
    own_sem,
    near_sem,
    pass_sem,
    far_sem,
    last_sem,
    done_sem,
):
    matrices, rows, columns = out.shape
    tokens = abuf.shape[1]
    blocks = columns // BLOCK
    pieces = matrices * blocks
    half = rows // 2
    chunk = half // chips
    h = chunk // 2

    me = lax.axis_index("dp")
    chip, core = me // 2, me % 2
    other = chip * 2 + 1 - core
    nxt, prv = (chip + 1) % chips, (chip + chips - 1) % chips
    opp = (chip + 2) % chips
    right, left = nxt * 2 + core, prv * 2 + core
    to = (right, left)
    beside = (nxt, prv)

    class Piece:
        def __init__(self, p):
            self.p = p
            self.n = p // blocks
            self.acc = p % ACCS
            self.cols = pl.ds(pl.multiple_of(p % blocks * BLOCK, BLOCK), BLOCK)

        def in_out(self, row, size):
            return out.at[self.n, pl.ds(pl.multiple_of(core * half + row, h), size), self.cols]

    def a_copy(n):
        return pltpu.make_async_copy(a_hbm.at[0, n], abuf.at[n % 2], a_sem.at[n % 2])

    def g_copy(p):
        cols = pl.ds(pl.multiple_of(p % blocks * BLOCK, BLOCK), BLOCK)
        return pltpu.make_async_copy(g_hbm.at[0, p // blocks, :, cols], gbuf.at[p % 3], g_sem.at[p % 3])

    def head_part(k):
        unit = tokens // sum(HEAD)
        return pl.ds(sum(HEAD[:k]) * unit, HEAD[k] * unit)

    def head_copies(k):
        some = head_part(k)
        return (
            pltpu.make_async_copy(a_hbm.at[0, 0, some], abuf.at[0, some], head_sem.at[k]),
            pltpu.make_async_copy(g_hbm.at[0, 0, some, pl.ds(0, BLOCK)], gbuf.at[0, some], head_sem.at[k]),
        )

    def send(src, dst, send_sem, recv_sem, device):
        return pltpu.make_async_remote_copy(
            src_ref=src,
            dst_ref=dst,
            send_sem=send_sem,
            recv_sem=recv_sem,
            device_id={"dp": device},
            device_id_type=MESH,
        )

    def rows_of(row, size):
        return pl.ds(pl.multiple_of(row, h), size)

    def exchange(x):
        return send(give.at[x.p], take.at[x.p], give_sem, take_sem.at[x.p % 3], other)

    def part_copy(x, way):
        src = stage.at[x.p, pl.ds(2 * chunk + way * h, h)]
        return send(src, part.at[x.p, way], stage_sem, part_sem.at[x.p % PARTS], to[way])

    def whole_copy(x, way, piece_half):
        src = stage.at[x.p, pl.ds(way * chunk + piece_half * h, h)]
        dst = whole.at[x.p, way, pl.ds(piece_half * h, h)]
        return send(src, dst, stage_sem, whole_sem.at[x.p % WHOLES], to[way])

    def own_copy(x, way):
        where = x.in_out(chip * chunk, chunk)
        return send(where, where, own_sem, near_sem.at[x.p // 2], to[way])

    def pass_copy(x, way):
        where = x.in_out((prv, nxt)[way] * chunk + way * h, h)
        return send(where, where, pass_sem, far_sem.at[x.p // 2], to[way])

    def last_copy(x, owner):
        where = x.in_out(owner * chunk, chunk)
        return send(where, where, last_sem, done_sem, other)

    def wait_all(ref, sem):
        pltpu.make_async_copy(ref, ref, sem).wait()

    def own_term(x, row, size):
        where = rows_of(row, size)
        return acc[x.acc, where] + take[x.p, where].astype(jnp.float32)

    def begin(x):
        exchange(x).wait_recv()
        stage[x.p, pl.ds(2 * chunk, chunk)] = own_term(x, opp * chunk, chunk).astype(stage.dtype)
        for way in range(2):
            part_copy(x, way).start()
        for way in range(2):
            rest = beside[way] * chunk + (1 - way) * h
            stage[x.p, pl.ds(way * chunk + (1 - way) * h, h)] = own_term(x, rest, h).astype(stage.dtype)
            whole_copy(x, way, 1 - way).start()
        for way in range(2):
            row = beside[way] * chunk + way * h
            acc[x.acc, rows_of(row, h)] = own_term(x, row, h)
        kept[x.p] = own_term(x, chip * chunk, chunk)

    def pass_parts(x):
        wait_all(part.at[x.p], part_sem.at[x.p % PARTS])
        for way in range(2):
            mine = acc[x.acc, rows_of(beside[way] * chunk + way * h, h)]
            total = mine + part[x.p, way].astype(jnp.float32)
            stage[x.p, pl.ds(way * chunk + way * h, h)] = total.astype(stage.dtype)
            whole_copy(x, way, way).start()

    def finish(x):
        wait_all(whole.at[x.p], whole_sem.at[x.p % WHOLES])
        total = kept[x.p]
        for way in range(2):
            total += whole[x.p, way].astype(jnp.float32)
        x.in_out(chip * chunk, chunk)[...] = total.astype(out.dtype)
        for way in range(2):
            own_copy(x, way).start()

    def gather(q):
        wait_all(whole.at[pl.ds(2 * q, 2)], near_sem.at[q])
        for x in (Piece(2 * q), Piece(2 * q + 1)):
            for way in range(2):
                pass_copy(x, way).start()
            for owner in (chip, nxt, prv):
                last_copy(x, owner).start()

    def close(q):
        wait_all(part.at[pl.ds(2 * q, 2)], far_sem.at[q])
        for x in (Piece(2 * q), Piece(2 * q + 1)):
            last_copy(x, opp).start()

    def when(live, do, p):
        pl.when(live & (p >= 0) & (p < pieces))(lambda: do(Piece(p)))

    def product(lhs, rhs):
        return lax.dot_general(lhs, rhs, (((0,), (0,)), ((), ())), preferred_element_type=jnp.float32)

    for k in range(len(HEAD)):
        for copy in head_copies(k):
            copy.start()
    g_copy(1).start()
    barrier = pltpu.get_barrier_semaphore()
    for device in (other, right, left):
        pl.semaphore_signal(barrier, inc=1, device_id={"dp": device}, device_id_type=MESH)
    mine, theirs = rows_of(core * half, half), rows_of((1 - core) * half, half)

    for k in range(len(HEAD)):
        some = head_part(k)
        wait_all(gbuf.at[pl.ds(0, 2), some], head_sem.at[k])
        terms = product(abuf[0, some, theirs], gbuf[0, some])
        if k < len(HEAD) - 1:
            acc[1] = terms + acc[1] if k else terms
        else:
            give[0] = (terms + acc[1]).astype(give.dtype)
            pl.semaphore_wait(barrier, 3)
            exchange(Piece(0)).start()
        terms = product(abuf[0, some, mine], gbuf[0, some])
        acc[0] = terms + acc[0] if k else terms
    g_copy(2).start()

    @pl.loop(1, CLOSE + pieces // 2)
    def _(s):
        p, n, c = s, s // blocks, s % blocks

        @pl.when(s < pieces)
        def _():
            @pl.when(p + 2 < pieces)
            def _():
                g_copy(p + 2).start()

            @pl.when((c == 1) & (n + 1 < matrices))
            def _():
                a_copy(n + 1).start()

            @pl.when(c == 0)
            def _():
                a_copy(n).wait()

            g_copy(p).wait()
            give[p] = product(abuf[n % 2, :, theirs], gbuf[p % 3]).astype(give.dtype)
            exchange(Piece(p)).start()

        when(s == 1, begin, 0)
        when(s > 2, pass_parts, s - 2)
        when(s == 4, finish, 0)

        @pl.when(s < pieces)
        def _():
            acc[p % ACCS] = product(abuf[n % 2, :, mine], gbuf[p % 3])

        when(s == 2, pass_parts, 0)
        when(s > 0, begin, s)
        k = s - SPARSE
        when((s < DENSE[0]) & (k > 0) & (k % 3 != 0), finish, k - k // 3)
        first = DENSE[0] - SPARSE
        for i in range(DENSE[1]):
            when(s >= DENSE[0], finish, first - (first + 2) // 3 + 1 + (s - DENSE[0]) * DENSE[1] + i)
        pl.when((s >= GATHER) & (s < GATHER + pieces // 2))(lambda: gather(s - GATHER))
        pl.when(s >= CLOSE)(lambda: close(s - CLOSE))

    wait_all(give, give_sem)
    wait_all(stage, stage_sem)
    wait_all(whole, own_sem)
    wait_all(part, pass_sem)
    wait_all(take, last_sem)
    wait_all(take, done_sem)


def solution(mesh):
    chips = mesh.shape["dp"] // 2

    def step(a, g):
        _, matrices, tokens, rows = a.shape
        columns = g.shape[-1]
        pieces = matrices * (columns // BLOCK)
        half = rows // 2
        chunk = half // chips
        vmem = lambda *shape: pltpu.VMEM(shape, jnp.bfloat16)
        dma = pltpu.SemaphoreType.DMA
        return pl.pallas_call(
            functools.partial(kernel, chips),
            out_shape=pltpu.VMEM((matrices, rows, columns), jnp.bfloat16),
            in_specs=[pl.BlockSpec(memory_space=pl.ANY)] * 2,
            out_specs=pl.BlockSpec(memory_space=pltpu.VMEM),
            scratch_shapes=[
                vmem(2, tokens, rows),
                vmem(3, tokens, BLOCK),
                pltpu.VMEM((ACCS, half, BLOCK), jnp.float32),
                pltpu.VMEM((pieces, chunk, BLOCK), jnp.float32),
                vmem(pieces, half, BLOCK),
                vmem(pieces, half, BLOCK),
                vmem(pieces, 3 * chunk, BLOCK),
                vmem(pieces, 2, chunk // 2, BLOCK),
                vmem(pieces, 2, chunk, BLOCK),
                dma((len(HEAD),)),
                dma((2,)),
                dma((3,)),
                dma,
                dma((3,)),
                dma,
                dma((PARTS,)),
                dma((WHOLES,)),
                dma,
                dma((pieces // 2,)),
                dma,
                dma((pieces // 2,)),
                dma,
                dma,
            ],
            compiler_params=pltpu.CompilerParams(
                collective_id=0, has_side_effects=True, vmem_limit_bytes=50 * 2**20
            ),
            name="grad_sums",
        )(a, g)

    return jax.shard_map(
        step,
        mesh=mesh,
        in_specs=(P(("rep", "dp")), P(("rep", "dp"))),
        out_specs=P("rep"),
        check_vma=False,
    )
```

```python
import functools

import jax
import jax.numpy as jnp
from jax import lax
from jax.experimental import pallas as pl
from jax.experimental.pallas import tpu as pltpu
from jax.sharding import PartitionSpec as P

MESH = pl.DeviceIdType.MESH
BLOCK = 512
ACCS = 4
HEAD = 2, 2, 2, 2
PARTS, WHOLES = 6, 9
SPARSE = 3
DENSE = 15, 2
GATHER = 18
CLOSE = 21

def kernel(
    chips,
    a_hbm,
    g_hbm,
    out,
    abuf,
    gbuf,
    acc,
    kept,
    give,
    take,
    stage,
    part,
    whole,
    head_sem,
    a_sem,
    g_sem,
    give_sem,
    take_sem,
    stage_sem,
    part_sem,
    whole_sem,
    own_sem,
    near_sem,
    pass_sem,
    far_sem,
    last_sem,
    done_sem,
):
    matrices, rows, columns = out.shape
    tokens = abuf.shape[1]
    blocks = columns // BLOCK
    pieces = matrices * blocks
    half = rows // 2
    chunk = half // chips
    h = chunk // 2

    me = lax.axis_index("dp")
    chip, core = me // 2, me % 2
    other = chip * 2 + 1 - core
    nxt, prv = (chip + 1) % chips, (chip + chips - 1) % chips
    opp = (chip + 2) % chips
    right, left = nxt * 2 + core, prv * 2 + core
    to = (right, left)
    beside = (nxt, prv)

    class Piece:
        def __init__(self, p):
            self.p = p
            self.n = p // blocks
            self.acc = p % ACCS
            self.cols = pl.ds(pl.multiple_of(p % blocks * BLOCK, BLOCK), BLOCK)

        def in_out(self, row, size):
            return out.at[self.n, pl.ds(pl.multiple_of(core * half + row, h), size), self.cols]

    def a_copy(n):
        return pltpu.make_async_copy(a_hbm.at[0, n], abuf.at[n % 2], a_sem.at[n % 2])

    def g_copy(p):
        cols = pl.ds(pl.multiple_of(p % blocks * BLOCK, BLOCK), BLOCK)
        return pltpu.make_async_copy(g_hbm.at[0, p // blocks, :, cols], gbuf.at[p % 3], g_sem.at[p % 3])

    def head_part(k):
        unit = tokens // sum(HEAD)
        return pl.ds(sum(HEAD[:k]) * unit, HEAD[k] * unit)

    def head_copies(k):
        some = head_part(k)
        return (
            pltpu.make_async_copy(a_hbm.at[0, 0, some], abuf.at[0, some], head_sem.at[k]),
            pltpu.make_async_copy(g_hbm.at[0, 0, some, pl.ds(0, BLOCK)], gbuf.at[0, some], head_sem.at[k]),
        )

    def second_copy(k):
        some = pl.ds(k * (tokens // 2), tokens // 2)
        g = g_hbm.at[0, 0, some, pl.ds(BLOCK, BLOCK)]
        return pltpu.make_async_copy(g, gbuf.at[1, some], (g_sem.at[1], a_sem.at[0])[k])

    def send(src, dst, send_sem, recv_sem, device):
        return pltpu.make_async_remote_copy(
            src_ref=src,
            dst_ref=dst,
            send_sem=send_sem,
            recv_sem=recv_sem,
            device_id={"dp": device},
            device_id_type=MESH,
        )

    def rows_of(row, size):
        return pl.ds(pl.multiple_of(row, h), size)

    def exchange(x):
        return send(give.at[x.p], take.at[x.p], give_sem, take_sem.at[x.p % 3], other)

    def part_copy(x, way):
        src = stage.at[x.p, pl.ds(2 * chunk + way * h, h)]
        return send(src, part.at[x.p, way], stage_sem, part_sem.at[x.p % PARTS], to[way])

    def whole_copy(x, way, piece_half):
        src = stage.at[x.p, pl.ds(way * chunk + piece_half * h, h)]
        dst = whole.at[x.p, way, pl.ds(piece_half * h, h)]
        return send(src, dst, stage_sem, whole_sem.at[x.p % WHOLES], to[way])

    def own_copy(x, way):
        where = x.in_out(chip * chunk, chunk)
        return send(where, where, own_sem, near_sem.at[x.p // 2], to[way])

    def pass_copy(x, way):
        where = x.in_out((prv, nxt)[way] * chunk + way * h, h)
        return send(where, where, pass_sem, far_sem.at[x.p // 2], to[way])

    def last_copy(x, owner):
        where = x.in_out(owner * chunk, chunk)
        return send(where, where, last_sem, done_sem, other)

    def wait_all(ref, sem):
        pltpu.make_async_copy(ref, ref, sem).wait()

    def own_term(x, row, size):
        where = rows_of(row, size)
        return acc[x.acc, where] + take[x.p, where].astype(jnp.float32)

    def begin(x):
        exchange(x).wait_recv()
        stage[x.p, pl.ds(2 * chunk, chunk)] = own_term(x, opp * chunk, chunk).astype(stage.dtype)
        for way in range(2):
            part_copy(x, way).start()
        for way in range(2):
            rest = beside[way] * chunk + (1 - way) * h
            stage[x.p, pl.ds(way * chunk + (1 - way) * h, h)] = own_term(x, rest, h).astype(stage.dtype)
            whole_copy(x, way, 1 - way).start()

    def pass_parts(x):
        wait_all(part.at[x.p], part_sem.at[x.p % PARTS])
        for way in range(2):
            total = own_term(x, beside[way] * chunk + way * h, h) + part[x.p, way].astype(jnp.float32)
            stage[x.p, pl.ds(way * chunk + way * h, h)] = total.astype(stage.dtype)
            whole_copy(x, way, way).start()
        kept[x.p] = own_term(x, chip * chunk, chunk)

    def finish(x):
        wait_all(whole.at[x.p], whole_sem.at[x.p % WHOLES])
        total = kept[x.p]
        for way in range(2):
            total += whole[x.p, way].astype(jnp.float32)
        x.in_out(chip * chunk, chunk)[...] = total.astype(out.dtype)
        for way in range(2):
            own_copy(x, way).start()

    def gather(q):
        wait_all(whole.at[pl.ds(2 * q, 2)], near_sem.at[q])
        for x in (Piece(2 * q), Piece(2 * q + 1)):
            for way in range(2):
                pass_copy(x, way).start()
            for owner in (chip, nxt, prv):
                last_copy(x, owner).start()

    def close(q):
        wait_all(part.at[pl.ds(2 * q, 2)], far_sem.at[q])
        for x in (Piece(2 * q), Piece(2 * q + 1)):
            last_copy(x, opp).start()

    def when(live, do, p):
        pl.when(live & (p >= 0) & (p < pieces))(lambda: do(Piece(p)))

    def product(lhs, rhs):
        return lax.dot_general(lhs, rhs, (((0,), (0,)), ((), ())), preferred_element_type=jnp.float32)

    for k in range(len(HEAD)):
        for copy in head_copies(k):
            copy.start()
    for k in range(2):
        second_copy(k).start()
    barrier = pltpu.get_barrier_semaphore()
    for device in (other, right, left):
        pl.semaphore_signal(barrier, inc=1, device_id={"dp": device}, device_id_type=MESH)
    mine, theirs = rows_of(core * half, half), rows_of((1 - core) * half, half)

    for k in range(len(HEAD)):
        some = head_part(k)
        wait_all(gbuf.at[pl.ds(0, 2), some], head_sem.at[k])
        terms = product(abuf[0, some, theirs], gbuf[0, some])
        if k < len(HEAD) - 1:
            acc[1] = terms + acc[1] if k else terms
        else:
            give[0] = (terms + acc[1]).astype(give.dtype)
            pl.semaphore_wait(barrier, 3)
            exchange(Piece(0)).start()
        terms = product(abuf[0, some, mine], gbuf[0, some])
        acc[0] = terms + acc[0] if k else terms
    g_copy(2).start()

    low, high = pl.ds(0, tokens // 2), pl.ds(tokens // 2, tokens // 2)
    second_copy(0).wait()
    acc[1] = product(abuf[0, low, theirs], gbuf[1, low])
    second_copy(1).wait()
    give[1] = (acc[1] + product(abuf[0, high, theirs], gbuf[1, high])).astype(give.dtype)
    exchange(Piece(1)).start()
    begin(Piece(0))
    g_copy(3).start()
    a_copy(1).start()
    acc[1] = product(abuf[0, :, mine], gbuf[1])
    begin(Piece(1))

    @pl.loop(2, CLOSE + pieces // 2)
    def _(s):
        p, n, c = s, s // blocks, s % blocks

        @pl.when(s < pieces)
        def _():
            @pl.when(p + 2 < pieces)
            def _():
                g_copy(p + 2).start()

            @pl.when((c == 1) & (n + 1 < matrices))
            def _():
                a_copy(n + 1).start()

            @pl.when(c == 0)
            def _():
                a_copy(n).wait()

            g_copy(p).wait()
            give[p] = product(abuf[n % 2, :, theirs], gbuf[p % 3]).astype(give.dtype)
            exchange(Piece(p)).start()

        when(s > 2, pass_parts, s - 2)
        when(s == 4, finish, 0)

        @pl.when(s < pieces)
        def _():
            acc[p % ACCS] = product(abuf[n % 2, :, mine], gbuf[p % 3])

        when(s == 2, pass_parts, 0)
        when(s > 0, begin, s)
        k = s - SPARSE
        when((s < DENSE[0]) & (k > 0) & (k % 3 != 0), finish, k - k // 3)
        first = DENSE[0] - SPARSE
        for i in range(DENSE[1]):
            when(s >= DENSE[0], finish, first - (first + 2) // 3 + 1 + (s - DENSE[0]) * DENSE[1] + i)
        pl.when((s >= GATHER) & (s < GATHER + pieces // 2))(lambda: gather(s - GATHER))
        pl.when(s >= CLOSE)(lambda: close(s - CLOSE))

    wait_all(give, give_sem)
    wait_all(stage, stage_sem)
    wait_all(whole, own_sem)
    wait_all(part, pass_sem)
    wait_all(take, last_sem)
    wait_all(take, done_sem)


def solution(mesh):
    chips = mesh.shape["dp"] // 2

    def step(a, g):
        _, matrices, tokens, rows = a.shape
        columns = g.shape[-1]
        pieces = matrices * (columns // BLOCK)
        half = rows // 2
        chunk = half // chips
        vmem = lambda *shape: pltpu.VMEM(shape, jnp.bfloat16)
        dma = pltpu.SemaphoreType.DMA
        return pl.pallas_call(
            functools.partial(kernel, chips),
            out_shape=pltpu.VMEM((matrices, rows, columns), jnp.bfloat16),
            in_specs=[pl.BlockSpec(memory_space=pl.ANY)] * 2,
            out_specs=pl.BlockSpec(memory_space=pltpu.VMEM),
            scratch_shapes=[
                vmem(2, tokens, rows),
                vmem(3, tokens, BLOCK),
                pltpu.VMEM((ACCS, half, BLOCK), jnp.float32),
                pltpu.VMEM((pieces, chunk, BLOCK), jnp.float32),
                vmem(pieces, half, BLOCK),
                vmem(pieces, half, BLOCK),
                vmem(pieces, 3 * chunk, BLOCK),
                vmem(pieces, 2, chunk // 2, BLOCK),
                vmem(pieces, 2, chunk, BLOCK),
                dma((len(HEAD),)),
                dma((2,)),
                dma((3,)),
                dma,
                dma((3,)),
                dma,
                dma((PARTS,)),
                dma((WHOLES,)),
                dma,
                dma((pieces // 2,)),
                dma,
                dma((pieces // 2,)),
                dma,
                dma,
            ],
            compiler_params=pltpu.CompilerParams(
                collective_id=0, has_side_effects=True, vmem_limit_bytes=50 * 2**20
            ),
            name="grad_sums",
        )(a, g)

    return jax.shard_map(
        step,
        mesh=mesh,
        in_specs=(P(("rep", "dp")), P(("rep", "dp"))),
        out_specs=P("rep"),
        check_vma=False,
    )
```

```python
import functools

import jax
import jax.numpy as jnp
from jax import lax
from jax.experimental import pallas as pl
from jax.experimental.pallas import tpu as pltpu
from jax.sharding import PartitionSpec as P

MESH = pl.DeviceIdType.MESH
BLOCK = 512
ACCS = 4
HEAD = 2, 2, 2, 2
PARTS, WHOLES = 6, 9
SPARSE = 3
DENSE = 15, 2
GATHER = 18
YIELD = 2
CLOSE = 21

def kernel(
    chips,
    a_hbm,
    g_hbm,
    out,
    abuf,
    gbuf,
    acc,
    kept,
    give,
    take,
    stage,
    part,
    whole,
    head_sem,
    a_sem,
    g_sem,
    give_sem,
    take_sem,
    stage_sem,
    part_sem,
    whole_sem,
    own_sem,
    near_sem,
    pass_sem,
    far_sem,
    last_sem,
    done_sem,
):
    matrices, rows, columns = out.shape
    tokens = abuf.shape[1]
    blocks = columns // BLOCK
    pieces = matrices * blocks
    half = rows // 2
    chunk = half // chips
    h = chunk // 2

    me = lax.axis_index("dp")
    chip, core = me // 2, me % 2
    other = chip * 2 + 1 - core
    nxt, prv = (chip + 1) % chips, (chip + chips - 1) % chips
    opp = (chip + 2) % chips
    right, left = nxt * 2 + core, prv * 2 + core
    to = (right, left)
    beside = (nxt, prv)

    class Piece:
        def __init__(self, p):
            self.p = p
            self.n = p // blocks
            self.acc = p % ACCS
            self.cols = pl.ds(pl.multiple_of(p % blocks * BLOCK, BLOCK), BLOCK)

        def in_out(self, row, size):
            return out.at[self.n, pl.ds(pl.multiple_of(core * half + row, h), size), self.cols]

    def a_copy(n):
        return pltpu.make_async_copy(a_hbm.at[0, n], abuf.at[n % 2], a_sem.at[n % 2])

    def g_copy(p):
        cols = pl.ds(pl.multiple_of(p % blocks * BLOCK, BLOCK), BLOCK)
        return pltpu.make_async_copy(g_hbm.at[0, p // blocks, :, cols], gbuf.at[p % 3], g_sem.at[p % 3])

    def head_part(k):
        unit = tokens // sum(HEAD)
        return pl.ds(sum(HEAD[:k]) * unit, HEAD[k] * unit)

    def head_copies(k):
        some = head_part(k)
        return (
            pltpu.make_async_copy(a_hbm.at[0, 0, some], abuf.at[0, some], head_sem.at[k]),
            pltpu.make_async_copy(g_hbm.at[0, 0, some, pl.ds(0, BLOCK)], gbuf.at[0, some], head_sem.at[k]),
        )

    def second_copy(k):
        some = pl.ds(k * (tokens // 2), tokens // 2)
        g = g_hbm.at[0, 0, some, pl.ds(BLOCK, BLOCK)]
        return pltpu.make_async_copy(g, gbuf.at[1, some], (g_sem.at[1], a_sem.at[0])[k])

    def send(src, dst, send_sem, recv_sem, device):
        return pltpu.make_async_remote_copy(
            src_ref=src,
            dst_ref=dst,
            send_sem=send_sem,
            recv_sem=recv_sem,
            device_id={"dp": device},
            device_id_type=MESH,
        )

    def rows_of(row, size):
        return pl.ds(pl.multiple_of(row, h), size)

    def exchange(x):
        return send(give.at[x.p], take.at[x.p], give_sem, take_sem.at[x.p % 3], other)

    def part_copy(x, way):
        src = stage.at[x.p, pl.ds(2 * chunk + way * h, h)]
        return send(src, part.at[x.p, way], stage_sem, part_sem.at[x.p % PARTS], to[way])

    def whole_copy(x, way, piece_half):
        src = stage.at[x.p, pl.ds(way * chunk + piece_half * h, h)]
        dst = whole.at[x.p, way, pl.ds(piece_half * h, h)]
        return send(src, dst, stage_sem, whole_sem.at[x.p % WHOLES], to[way])

    def own_copy(x, way):
        where = x.in_out(chip * chunk, chunk)
        return send(where, where, own_sem, near_sem.at[x.p // 2], to[way])

    def pass_copy(x, way):
        where = x.in_out((prv, nxt)[way] * chunk + way * h, h)
        return send(where, where, pass_sem, far_sem.at[x.p // 2], to[way])

    def last_copy(x, owner):
        where = x.in_out(owner * chunk, chunk)
        return send(where, where, last_sem, done_sem, other)

    def wait_all(ref, sem):
        pltpu.make_async_copy(ref, ref, sem).wait()

    def own_term(x, row, size):
        where = rows_of(row, size)
        return acc[x.acc, where] + take[x.p, where].astype(jnp.float32)

    def begin(x):
        exchange(x).wait_recv()
        stage[x.p, pl.ds(2 * chunk, chunk)] = own_term(x, opp * chunk, chunk).astype(stage.dtype)
        for way in range(2):
            part_copy(x, way).start()
        for way in range(2):
            rest = beside[way] * chunk + (1 - way) * h
            stage[x.p, pl.ds(way * chunk + (1 - way) * h, h)] = own_term(x, rest, h).astype(stage.dtype)
            whole_copy(x, way, 1 - way).start()

    def pass_parts(x):
        wait_all(part.at[x.p], part_sem.at[x.p % PARTS])
        for way in range(2):
            total = own_term(x, beside[way] * chunk + way * h, h) + part[x.p, way].astype(jnp.float32)
            stage[x.p, pl.ds(way * chunk + way * h, h)] = total.astype(stage.dtype)
            whole_copy(x, way, way).start()
        kept[x.p] = own_term(x, chip * chunk, chunk)

    def finish(x):
        wait_all(whole.at[x.p], whole_sem.at[x.p % WHOLES])
        total = kept[x.p]
        for way in range(2):
            total += whole[x.p, way].astype(jnp.float32)
        x.in_out(chip * chunk, chunk)[...] = total.astype(out.dtype)
        for way in range(2):
            own_copy(x, way).start()

    def gather(q):
        wait_all(whole.at[pl.ds(2 * q, 2)], near_sem.at[q])
        for x in (Piece(2 * q), Piece(2 * q + 1)):
            for way in range(2):
                pass_copy(x, way).start()
            for owner in (chip, nxt, prv):
                last_copy(x, owner).start()

    def close(q):
        wait_all(part.at[pl.ds(2 * q, 2)], far_sem.at[q])
        for x in (Piece(2 * q), Piece(2 * q + 1)):
            last_copy(x, opp).start()

    def when(live, do, p):
        pl.when(live & (p >= 0) & (p < pieces))(lambda: do(Piece(p)))

    def product(lhs, rhs):
        return lax.dot_general(lhs, rhs, (((0,), (0,)), ((), ())), preferred_element_type=jnp.float32)

    for k in range(len(HEAD)):
        for copy in head_copies(k):
            copy.start()
    for k in range(2):
        second_copy(k).start()
    barrier = pltpu.get_barrier_semaphore()
    for device in (other, right, left):
        pl.semaphore_signal(barrier, inc=1, device_id={"dp": device}, device_id_type=MESH)
    mine, theirs = rows_of(core * half, half), rows_of((1 - core) * half, half)

    for k in range(len(HEAD)):
        some = head_part(k)
        wait_all(gbuf.at[pl.ds(0, 2), some], head_sem.at[k])
        terms = product(abuf[0, some, theirs], gbuf[0, some])
        if k < len(HEAD) - 1:
            acc[1] = terms + acc[1] if k else terms
        else:
            give[0] = (terms + acc[1]).astype(give.dtype)
            pl.semaphore_wait(barrier, 3)
            exchange(Piece(0)).start()
        terms = product(abuf[0, some, mine], gbuf[0, some])
        acc[0] = terms + acc[0] if k else terms
    g_copy(2).start()

    low, high = pl.ds(0, tokens // 2), pl.ds(tokens // 2, tokens // 2)
    second_copy(0).wait()
    acc[1] = product(abuf[0, low, theirs], gbuf[1, low])
    second_copy(1).wait()
    give[1] = (acc[1] + product(abuf[0, high, theirs], gbuf[1, high])).astype(give.dtype)
    exchange(Piece(1)).start()
    begin(Piece(0))
    g_copy(3).start()
    a_copy(1).start()
    acc[1] = product(abuf[0, :, mine], gbuf[1])
    begin(Piece(1))

    @pl.loop(2, CLOSE + pieces // 2)
    def _(s):
        p, n, c = s, s // blocks, s % blocks

        @pl.when(s < pieces)
        def _():
            @pl.when(p + 2 < pieces)
            def _():
                g_copy(p + 2).start()

            @pl.when((c == 1) & (n + 1 < matrices))
            def _():
                a_copy(n + 1).start()

            @pl.when(c == 0)
            def _():
                a_copy(n).wait()

            g_copy(p).wait()
            give[p] = product(abuf[n % 2, :, theirs], gbuf[p % 3]).astype(give.dtype)
            exchange(Piece(p)).start()

        when(s > 2, pass_parts, s - 2)
        when(s == 4, finish, 0)

        @pl.when(s < pieces)
        def _():
            acc[p % ACCS] = product(abuf[n % 2, :, mine], gbuf[p % 3])

        when(s == 2, pass_parts, 0)
        when(s > 0, begin, s)
        k = s - SPARSE
        when((s < DENSE[0]) & (k > 0) & (k % 3 != 0), finish, k - k // 3)
        first = DENSE[0] - SPARSE
        for i in range(DENSE[1]):
            when(s >= DENSE[0], finish, first - (first + 2) // 3 + 1 + (s - DENSE[0]) * DENSE[1] + i)
        final = pieces // 2 - 1
        pl.when((s >= GATHER) & (s < GATHER + final))(lambda: gather(s - GATHER))
        pl.when(s == GATHER + final + core * YIELD)(lambda: gather(final))
        pl.when(s >= CLOSE)(lambda: close(s - CLOSE))

    wait_all(give, give_sem)
    wait_all(stage, stage_sem)
    wait_all(whole, own_sem)
    wait_all(part, pass_sem)
    wait_all(take, last_sem)
    wait_all(take, done_sem)


def solution(mesh):
    chips = mesh.shape["dp"] // 2

    def step(a, g):
        _, matrices, tokens, rows = a.shape
        columns = g.shape[-1]
        pieces = matrices * (columns // BLOCK)
        half = rows // 2
        chunk = half // chips
        vmem = lambda *shape: pltpu.VMEM(shape, jnp.bfloat16)
        dma = pltpu.SemaphoreType.DMA
        return pl.pallas_call(
            functools.partial(kernel, chips),
            out_shape=pltpu.VMEM((matrices, rows, columns), jnp.bfloat16),
            in_specs=[pl.BlockSpec(memory_space=pl.ANY)] * 2,
            out_specs=pl.BlockSpec(memory_space=pltpu.VMEM),
            scratch_shapes=[
                vmem(2, tokens, rows),
                vmem(3, tokens, BLOCK),
                pltpu.VMEM((ACCS, half, BLOCK), jnp.float32),
                pltpu.VMEM((pieces, chunk, BLOCK), jnp.float32),
                vmem(pieces, half, BLOCK),
                vmem(pieces, half, BLOCK),
                vmem(pieces, 3 * chunk, BLOCK),
                vmem(pieces, 2, chunk // 2, BLOCK),
                vmem(pieces, 2, chunk, BLOCK),
                dma((len(HEAD),)),
                dma((2,)),
                dma((3,)),
                dma,
                dma((3,)),
                dma,
                dma((PARTS,)),
                dma((WHOLES,)),
                dma,
                dma((pieces // 2,)),
                dma,
                dma((pieces // 2,)),
                dma,
                dma,
            ],
            compiler_params=pltpu.CompilerParams(
                collective_id=0, has_side_effects=True, vmem_limit_bytes=50 * 2**20
            ),
            name="grad_sums",
        )(a, g)

    return jax.shard_map(
        step,
        mesh=mesh,
        in_specs=(P(("rep", "dp")), P(("rep", "dp"))),
        out_specs=P("rep"),
        check_vma=False,
    )
```
